32 devices in a mesh: dp: 2 (over x), tp: 16 (over z, y, core).
Axes of the slice: x: 2, y: 2, z: 4, core: 2. Of those that a mesh axis runs over, the one named last changes fastest.
Arguments:
- query_hidden: bfloat16 [128, 8, 1024], P(('dp', 'tp')), parts along dimension 0
- doc_hidden: bfloat16 [128, 48, 1024], P(('dp', 'tp')), parts along dimension 0
- query_mask: int32 [128, 8], P(('dp', 'tp')), parts along dimension 0
- doc_mask: int32 [128, 48], P(('dp', 'tp')), parts along dimension 0
- positives: int32 [128], P(('dp', 'tp')), parts along dimension 0
- head_weight: bfloat16 [1024, 32768], P(None, 'tp')
- head_bias: float32 [1, 32768], P(None, 'tp')
Outputs:
- output 1: float32 [2], P('dp'), parts along dimension 0
- output 2: bfloat16 [2048, 32768], P('dp', 'tp'), parts along dimension 0
- output 3: float32 [2, 32768], P('dp', 'tp'), parts along dimension 0
- output 4: bfloat16 [128, 8, 1024], P(('dp', 'tp')), parts along dimension 0
- output 5: bfloat16 [128, 48, 1024], P(('dp', 'tp')), parts along dimension 0
There are 2 independent parts. The reference program is written for one: setup_inputs(seed, part) draws one part's arguments, and reference() takes and returns one part's arrays. A program takes and returns all parts, laid end to end along the dimension named above; an argument that names none is the same for every part.
All inputs are finite; a program needn't handle non-finite values.
Results may differ from the reference program's by a relative error of at most 0.010234.
Values are sent between devices in bfloat16 or wider.
A program may use at most 1 GiB of HBM per device.

```python
import math
import functools
import jax
import jax.numpy as jnp
from jax import lax

N_QUERIES = 64
N_DOCS = 64
Q_LEN = 8
D_LEN = 48
HIDDEN = 1024
VOCAB = 32768

QUERY_WEIGHT = math.sqrt(D_LEN) / (4.0 * math.sqrt(VOCAB) * Q_LEN)
DOC_WEIGHT = Q_LEN / (4.0 * math.sqrt(VOCAB) * D_LEN ** 1.5)


def draw_masks(rng_key, n_rows, length):
    len_key, row_key = jax.random.split(rng_key)
    lengths = jax.random.randint(len_key, (n_rows,), length // 2, length + 1)
    full_row = jax.random.randint(row_key, (), 0, n_rows)
    lengths = lengths.at[full_row].set(length)
    return (jnp.arange(length)[None, :] < lengths[:, None]).astype(jnp.int32)


def draw_positives(rng_key):
    pos_key, perm_key = jax.random.split(rng_key)
    positives = jax.random.randint(pos_key, (N_QUERIES,), 0, N_DOCS)
    perm_order = jax.random.permutation(perm_key, N_QUERIES)
    return positives.at[perm_order[0]].set(0).at[perm_order[1]].set(N_DOCS - 1)


def setup_inputs(seed: int = 0, part: int = 0) -> dict:
    shared = jax.random.split(jax.random.key(seed), 2)
    local_keys = jax.random.split(jax.random.fold_in(jax.random.key(seed + 1), part), 5)
    logit_scale = math.sqrt(12.0 / (math.sqrt(VOCAB) * Q_LEN * math.sqrt(D_LEN)))
    head_weight = (jax.random.normal(shared[0], (HIDDEN, VOCAB), jnp.float32) * (logit_scale / math.sqrt(HIDDEN))).astype(jnp.bfloat16)
    head_bias = jax.random.normal(shared[1], (1, VOCAB), jnp.float32) * (0.5 * logit_scale)
    query_hidden = jax.random.normal(local_keys[0], (N_QUERIES, Q_LEN, HIDDEN), jnp.float32).astype(jnp.bfloat16)
    doc_hidden = jax.random.normal(local_keys[1], (N_DOCS, D_LEN, HIDDEN), jnp.float32).astype(jnp.bfloat16)
    query_mask = draw_masks(local_keys[2], N_QUERIES, Q_LEN)
    doc_mask = draw_masks(local_keys[3], N_DOCS, D_LEN)
    positives = draw_positives(local_keys[4])
    return {'query_hidden': query_hidden, 'doc_hidden': doc_hidden, 'query_mask': query_mask, 'doc_mask': doc_mask, 'positives': positives, 'head_weight': head_weight, 'head_bias': head_bias}


def side_rep(hidden, token_mask, head_weight, head_bias):
    def one_row(row_args):
        hid_row, mask_row = row_args
        logits = jnp.dot(hid_row, head_weight, preferred_element_type=jnp.float32) + head_bias
        return jnp.sum(jnp.log1p(jnp.maximum(logits, 0.0)) * mask_row[:, None].astype(jnp.float32), axis=0)
    return lax.map(one_row, (hidden, token_mask))


def score_loss(rep_q, rep_d, positives):
    scores = jnp.dot(rep_q, rep_d.T, preferred_element_type=jnp.float32)
    target = positives[:, None] == jnp.arange(N_DOCS)[None, :]
    picked = jnp.sum(jnp.where(target, scores, 0.0), axis=1)
    cross = jnp.mean(jax.nn.logsumexp(scores, axis=1) - picked)
    mean_q = jnp.mean(rep_q, axis=0)
    mean_d = jnp.mean(rep_d, axis=0)
    return cross + QUERY_WEIGHT * jnp.sum(mean_q * mean_q) + DOC_WEIGHT * jnp.sum(mean_d * mean_d)


def side_back(hidden, token_mask, head_weight, head_bias, grad_rep):
    def body(carry, row_args):
        acc_weight, acc_bias = carry
        hid_row, mask_row, grad_row = row_args
        logits = jnp.dot(hid_row, head_weight, preferred_element_type=jnp.float32) + head_bias
        grad_gate = jnp.where(logits > 0.0, 1.0 / (1.0 + logits), 0.0) * mask_row[:, None].astype(jnp.float32)
        grad_logits = grad_row[None, :] * grad_gate
        grad_low = grad_logits.astype(jnp.bfloat16)
        acc_weight = acc_weight + jnp.dot(hid_row.T, grad_low, preferred_element_type=jnp.float32)
        acc_bias = acc_bias + jnp.sum(grad_logits, axis=0, keepdims=True)
        grad_hid = jnp.dot(grad_low, head_weight.T, preferred_element_type=jnp.float32).astype(jnp.bfloat16)
        return (acc_weight, acc_bias), grad_hid
    init = (jnp.zeros((HIDDEN, VOCAB), jnp.float32), jnp.zeros((1, VOCAB), jnp.float32))
    (acc_weight, acc_bias), grad_hidden = lax.scan(body, init, (hidden, token_mask, grad_rep))
    return acc_weight, acc_bias, grad_hidden


def reference(query_hidden, doc_hidden, query_mask, doc_mask, positives, head_weight, head_bias):
    rep_q = side_rep(query_hidden, query_mask, head_weight, head_bias)
    rep_d = side_rep(doc_hidden, doc_mask, head_weight, head_bias)
    loss_of = functools.partial(score_loss, positives=positives)
    total_loss, pull_back = jax.vjp(loss_of, rep_q, rep_d)
    grad_q, grad_d = pull_back(jnp.ones_like(total_loss))
    weight_q, bias_q, grad_query = side_back(query_hidden, query_mask, head_weight, head_bias, grad_q)
    weight_d, bias_d, grad_doc = side_back(doc_hidden, doc_mask, head_weight, head_bias, grad_d)
    grad_weight = (weight_q + weight_d).astype(jnp.bfloat16)
    return total_loss.reshape(1), grad_weight, bias_q + bias_d, grad_query, grad_doc
```

```python
import functools
import math
import jax
import jax.numpy as jnp
from jax import lax
from jax.experimental import pallas as pl
from jax.experimental.pallas import tpu as pltpu
from jax.sharding import PartitionSpec as P

HIGHEST = lax.Precision.HIGHEST
F32 = jnp.float32
BF16 = jnp.bfloat16
TILE = 256
ROWS = 4
NDEV = 16
NT_DIMS = (((1,), (1,)), ((), ()))
TN_DIMS = (((0,), (0,)), ((), ()))

END_AT = (3, 4, 6, 8, 9, 11, 13, 15)
MID_AT = (5, 6, 8, 9, 10, 11, 13, 15)


def kernel(d_len, q_len, lam_q, lam_d,
           xd, xq, md, mq, pos, w, b,
           loss, dw, db, dhd, dhq,
           hid_d, hid_q, meta, wv, hid_t, gate_d, gate_q, rep_d, rep_q, grad_d, grad_q,
           low, part, part_q, in_y, in_l, in_r, in_qz, in_qy, acc, pos_s, s_a, s_b,
           load_sem, meta_ss, meta_rs, qy_ss, qy_rs, qz_ss, qz_rs, qs_ss, qs_rs,
           dl_ss, dr_ss, dz_rs, dy_ss, dy_rs, ds_ss, ds_rs,
           sa_ss, sa_rs, sb_ss, sb_rs,
           bs_ss, bs_rs, by_ss, by_rs, bl_ss, br_ss, bl_rs, br_rs,
           cs_ss, cs_rs, cz_ss, cz_rs, cy_ss, cy_rs):
    n_pair = NDEV // 2
    rd, rq = ROWS * d_len, ROWS * q_len
    half = rd // 2
    hidden = wv.shape[0]
    tiles = wv.shape[1] // TILE
    n_q, n_d = NDEV * ROWS, NDEV * ROWS
    all_d = NDEV * rd
    me = lax.axis_index('tp')
    z, y, c = me // 4, (me // 2) % 2, me % 2
    far = z // 2
    mid = z * (1 - far) + (3 - z) * far
    sib = me + 1 - 2 * c
    over_y = me + 2 - 4 * y
    left, right = me - 4, me + 4

    def order(k):
        o = (k // 2) * k + (1 - k // 2) * ((k + mid) % 2)
        return o * (1 - far) + (3 - o) * far

    def remote(src, dst, ss, rs, dev):
        return pltpu.make_async_remote_copy(
            src_ref=src, dst_ref=dst, send_sem=ss, recv_sem=rs,
            device_id={'tp': dev}, device_id_type=pl.DeviceIdType.MESH)

    def got(dst, rs):
        remote(dst, dst, rs, rs, sib).wait_recv()

    def sent(src, ss):
        remote(src, src, ss, ss, sib).wait_send()

    load_d = pltpu.make_async_copy(xd, hid_d.at[me], load_sem.at[0])
    load_q = pltpu.make_async_copy(xq, hid_q.at[me // 2, c], load_sem.at[1])
    load_w = pltpu.make_async_copy(w, wv, load_sem.at[2])
    load_d.start()
    load_q.start()
    load_w.start()
    barrier = pltpu.get_barrier_semaphore()
    for j in range(1, NDEV):
        pl.semaphore_signal(barrier, inc=1, device_id={'tp': (me + j) % NDEV},
                            device_id_type=pl.DeviceIdType.MESH)
    row16 = lax.broadcasted_iota(jnp.int32, (16, TILE), 0)
    own_meta = jnp.zeros((16, TILE), F32)
    for r in range(ROWS):
        len_d = jnp.sum(md[r:r + 1, :].astype(F32), axis=1, keepdims=True)
        len_q = jnp.sum(mq[r:r + 1, :].astype(F32), axis=1, keepdims=True)
        own_meta = jnp.where(row16 == r, len_d, own_meta)
        own_meta = jnp.where(row16 == ROWS + r, len_q, own_meta)
        own_meta = jnp.where(row16 == 2 * ROWS + r, pos[r].astype(F32), own_meta)
    meta[me] = own_meta.astype(BF16)
    load_d.wait()
    load_q.wait()
    pl.semaphore_wait(barrier, NDEV - 1)

    def doc_half(shard, h):
        return hid_d.at[shard, pl.ds(h * half, half)]

    def pass_on(zs, h):
        ref = doc_half(4 * zs + 2 * y + c, h)
        remote(ref, ref, dy_ss.at[zs, h], dy_rs.at[zs, h], over_y).start()

        @pl.when(jnp.logical_and(zs >= z, z > 0))
        def _():
            remote(ref, ref, dl_ss.at[zs, h], dz_rs.at[zs, h], left).start()

        @pl.when(jnp.logical_and(zs <= z, z < 3))
        def _():
            remote(ref, ref, dr_ss.at[zs, h], dz_rs.at[zs, h], right).start()

        remote(ref, ref, ds_ss.at[2 * zs + y, h], ds_rs.at[2 * zs + y, h], sib).start()

    def arrive_line(zs):
        for h in range(2):
            got(doc_half(4 * zs + 2 * y + c, h), dz_rs.at[zs, h])
            pass_on(zs, h)

    def arrive_over(zs):
        p = 2 * zs + 1 - y
        for h in range(2):
            ref = doc_half(2 * p + c, h)
            got(ref, dy_rs.at[zs, h])
            remote(ref, ref, ds_ss.at[p, h], ds_rs.at[p, h], sib).start()

    def query_out(yy):
        ref = hid_q.at[2 * z + yy, c]
        for j in range(1, 4):
            remote(ref, ref, qz_ss.at[yy, j], qz_rs.at[z, yy], (me + 4 * j) % NDEV).start()

    for j in range(1, NDEV):
        remote(meta.at[me], meta.at[me], meta_ss.at[j], meta_rs.at[me], (me + j) % NDEV).start()
    own_q = hid_q.at[me // 2, c]
    pass_on(z, 0)
    remote(own_q, own_q, qy_ss.at[0], qy_rs.at[0], over_y).start()
    pass_on(z, 1)
    query_out(y)

    @pl.loop(1, NDEV)
    def _(j):
        src = (me + j) % NDEV
        got(meta.at[src], meta_rs.at[src])

    load_w.wait()

    def gated(logits, keep):
        on = jnp.logical_and(logits > 0.0, keep)
        held = jnp.where(on, logits, 0.0)
        up = 1.0 + held
        inv = 1.0 / up
        act = jnp.log(up) + (held - (up - 1.0)) * inv
        return act, jnp.where(on, inv, 0.0)

    place_d = lax.broadcasted_iota(jnp.int32, (d_len, TILE), 0).astype(F32)
    place_q = lax.broadcasted_iota(jnp.int32, (q_len, TILE), 0).astype(F32)

    def tile(n):
        return pl.ds(pl.multiple_of(n * TILE, TILE), TILE)

    def docs_forward(p):
        info = meta[pl.ds(2 * p, 2)].astype(F32)

        @pl.loop(0, tiles)
        def _(n):
            cols = tile(n)
            x = hid_d[pl.ds(2 * p, 2)].reshape(2 * rd, hidden)
            logits = jnp.dot(x, wv[:, cols], preferred_element_type=F32) + b[:, cols]
            for d in range(2 * ROWS):
                keep = place_d < info[d // ROWS, d % ROWS:d % ROWS + 1, :]
                act, gate = gated(logits[d_len * d:d_len * (d + 1)], keep)
                gate_d[pl.ds(p * 2 * rd + d_len * d, d_len), cols] = gate
                rep_d[pl.ds(p * 2 * ROWS + d, 1), cols] = jnp.sum(act, axis=0, keepdims=True)

        @pl.loop(0, hidden // 128)
        def _(t):
            lanes = pl.ds(pl.multiple_of(t * 128, 128), 128)
            block = hid_d[pl.ds(2 * p, 2), :, lanes].reshape(2 * rd, 128)
            hid_t[lanes, pl.ds(pl.multiple_of(p * 2 * rd, 128), 2 * rd)] = block.T

    def queries_forward():
        @pl.loop(0, tiles)
        def _(n):
            cols = tile(n)
            x = hid_q[...].reshape(NDEV * rq, hidden)
            logits = jnp.dot(x, wv[:, cols], preferred_element_type=F32) + b[:, cols]
            for i in range(NDEV):
                info = meta[i].astype(F32)
                for r in range(ROWS):
                    q = ROWS * i + r
                    keep = place_q < info[ROWS + r:ROWS + r + 1, :]
                    act, gate = gated(logits[q_len * q:q_len * (q + 1)], keep)
                    gate_q[q_len * q:q_len * (q + 1), cols] = gate
                    rep_q[q:q + 1, cols] = jnp.sum(act, axis=0, keepdims=True)

        @pl.loop(0, hidden // 128)
        def _(t):
            lanes = pl.ds(pl.multiple_of(t * 128, 128), 128)
            block = hid_q[:, :, :, lanes].reshape(NDEV * rq, 128)
            hid_t[lanes, all_d:all_d + NDEV * rq] = block.T

    def queries_pass():
        got(hid_q.at[2 * z + 1 - y, c], qy_rs.at[0])
        query_out(1 - y)

    def queries_share():
        for j in range(1, 4):
            zs = (z + j) % 4
            for yy in range(2):
                got(hid_q.at[2 * zs + yy, c], qz_rs.at[zs, yy])
        remote(hid_q.at[:, c], hid_q.at[:, c], qs_ss.at[0], qs_rs.at[0], sib).start()

    @pl.loop(0, 8)
    def _(u):
        k, other = u // 2, u % 2

        @pl.when(other == 1)
        def _():
            @pl.when(mid == 0)
            def _():
                @pl.when(k < 3)
                def _():
                    arrive_line(order(k + 1))

            @pl.when(mid == 1)
            def _():
                @pl.when(k == 0)
                def _():
                    queries_pass()
                    arrive_line(order(1))
                    arrive_line(order(2))

                @pl.when(k == 1)
                def _():
                    arrive_line(order(3))

            @pl.when(jnp.logical_and(mid == 0, k == 0))
            def _():
                queries_pass()

            arrive_over(order(k))

            @pl.when(k == 1)
            def _():
                queries_share()

        zs = order(k)
        p = 2 * zs + y + other * (1 - 2 * y)
        for h in range(2):
            got(doc_half(2 * p + 1 - c, h), ds_rs.at[p, h])
        docs_forward(p)

        @pl.when(u == 4)
        def _():
            got(hid_q.at[:, 1 - c], qs_rs.at[0])
            queries_forward()

    for j in range(1, NDEV):
        sent(meta.at[me], meta_ss.at[j])
    sent(own_q, qy_ss.at[0])
    for yy in range(2):
        for j in range(1, 4):
            sent(own_q, qz_ss.at[yy, j])
    sent(hid_q.at[:, c], qs_ss.at[0])
    for h in range(2):
        for zs in range(4):
            ref = doc_half(me, h)
            sent(ref, dy_ss.at[zs, h])

            @pl.when(jnp.logical_and(zs >= z, z > 0))
            def _():
                sent(ref, dl_ss.at[zs, h])

            @pl.when(jnp.logical_and(zs <= z, z < 3))
            def _():
                sent(ref, dr_ss.at[zs, h])
        for p in range(n_pair):
            sent(ref, ds_ss.at[p, h])

    mean_q = jnp.mean(rep_q[...], axis=0, keepdims=True)
    mean_d = jnp.mean(rep_d[...], axis=0, keepdims=True)
    reg = (lam_q * jnp.sum(mean_q * mean_q, axis=1, keepdims=True)
           + lam_d * jnp.sum(mean_d * mean_d, axis=1, keepdims=True))
    quad = 2 * y + c
    s_a[quad, :, 0:n_d] = lax.dot_general(rep_q[...], rep_d[...], NT_DIMS, precision=HIGHEST,
                                          preferred_element_type=F32)
    s_a[quad, :, n_d:2 * n_d] = jnp.broadcast_to(reg, (n_q, n_d))
    for j in range(1, 4):
        remote(s_a.at[quad], s_a.at[quad], sa_ss.at[j], sa_rs.at[quad], 4 * z + (quad + j) % 4).start()
    for i in range(NDEV):
        info = meta[i].astype(F32)
        pos_s[ROWS * i:ROWS * (i + 1), :] = info[2 * ROWS:3 * ROWS, 0:128]
    for j in range(1, 4):
        src = (quad + j) % 4
        got(s_a.at[src], sa_rs.at[src])
    s_b[z] = s_a[0] + s_a[1] + s_a[2] + s_a[3]
    for j in range(1, 4):
        remote(s_b.at[z], s_b.at[z], sb_ss.at[j], sb_rs.at[z], (me + 4 * j) % NDEV).start()
    for j in range(1, 4):
        src = (z + j) % 4
        got(s_b.at[src], sb_rs.at[src])
    total = s_b[0] + s_b[1] + s_b[2] + s_b[3]
    scores = total[:, 0:n_d]
    top = jnp.max(scores, axis=1, keepdims=True)
    log_norm = top + jnp.log(jnp.sum(jnp.exp(scores - top), axis=1, keepdims=True))
    lane = lax.broadcasted_iota(jnp.int32, (n_q, n_d), 1).astype(F32)
    target = (pos_s[:, 0:n_d] == lane).astype(F32)
    picked = jnp.sum(target * scores, axis=1, keepdims=True)
    cross = jnp.sum(log_norm - picked, axis=0, keepdims=True) / n_q
    loss[...] = cross + total[0:1, n_d:n_d + 1]
    grad_s = (jnp.exp(scores - log_norm) - target) / n_q

    @pl.loop(0, tiles)
    def _(n):
        cols = tile(n)
        rep_qn, rep_dn = rep_q[:, cols], rep_d[:, cols]
        grad_q[:, cols] = lax.dot_general(
            grad_s, rep_dn, (((1,), (0,)), ((), ())), precision=HIGHEST, preferred_element_type=F32
        ) + (2.0 * lam_q / n_q) * jnp.mean(rep_qn, axis=0, keepdims=True)
        grad_d[:, cols] = lax.dot_general(
            grad_s, rep_qn, TN_DIMS, precision=HIGHEST, preferred_element_type=F32
        ) + (2.0 * lam_d / n_d) * jnp.mean(rep_dn, axis=0, keepdims=True)

    db[...] = jnp.zeros_like(db)
    for j in range(1, 4):
        sent(s_a.at[0], sa_ss.at[j])
        sent(s_b.at[0], sb_ss.at[j])

    def pair_of(j):
        zs = order(3 - j // 2)
        other = 1 - j % 2
        return zs, 2 * zs + y + other * (1 - 2 * y)

    def hidden_grad(rows, store):
        @pl.loop(0, hidden // TILE)
        def _(t):
            hrows = tile(t)
            out = jnp.zeros((rows, TILE), F32)
            for n in range(tiles):
                out = out + lax.dot_general(
                    low[n * rows:(n + 1) * rows, :], wv[hrows, n * TILE:(n + 1) * TILE],
                    NT_DIMS, preferred_element_type=F32)
            store(hrows, out.astype(BF16))

    def docs_gate(p):
        rows = 2 * rd

        @pl.loop(0, tiles)
        def _(n):
            cols = tile(n)
            total_b = jnp.zeros((1, TILE), F32)
            for d in range(2 * ROWS):
                gz = grad_d[pl.ds(2 * ROWS * p + d, 1), cols] * gate_d[pl.ds(p * rows + d_len * d, d_len), cols]
                total_b = total_b + jnp.sum(gz, axis=0, keepdims=True)
                low[pl.ds(pl.multiple_of(n * rows + d_len * d, 16), d_len), :] = gz.astype(BF16)
            db[:, cols] += total_b

    def docs_hidden(slot):
        def store(hrows, out):
            part[slot, :, :, hrows] = out.reshape(2, rd, TILE)
        hidden_grad(2 * rd, store)

    def two_queries(q, cols):
        return jnp.concatenate(
            [grad_q[q + i:q + i + 1, cols] * gate_q[q_len * (q + i):q_len * (q + i + 1), cols]
             for i in range(2)], axis=0)

    def queries_back():
        rows = NDEV * rq

        @pl.loop(0, tiles)
        def _(n):
            cols = tile(n)
            total_b = jnp.zeros((1, TILE), F32)
            for q in range(0, n_q, 2):
                gz = two_queries(q, cols)
                total_b = total_b + jnp.sum(gz, axis=0, keepdims=True)
                low[pl.ds(pl.multiple_of(n * rows + q_len * q, 16), 2 * q_len), :] = gz.astype(BF16)
            db[:, cols] += total_b

        def store(hrows, out):
            part_q[:, :, :, hrows] = out.reshape(n_pair, 2, rq, TILE)
        hidden_grad(rows, store)
        remote(part_q.at[:, 1 - c], hid_q.at[:, 1], cs_ss.at[0], cs_rs.at[0], sib).start()

    def queries_chip():
        got(hid_q.at[:, 1], cs_rs.at[0])

        @pl.loop(0, n_pair)
        def _(p):
            hid_q[p, 0] = (part_q[p, c].astype(F32) + hid_q[p, 1].astype(F32)).astype(BF16)
        for j in range(1, 4):
            zs = (z + j) % 4
            remote(hid_q.at[pl.ds(2 * zs, 2), 0], in_qz.at[z], cz_ss.at[j], cz_rs.at[z],
                   (me + 4 * j) % NDEV).start()

    def queries_line():
        for j in range(1, 4):
            src = (z + j) % 4
            got(in_qz.at[src], cz_rs.at[src])
        for yy in range(2):
            p = 2 * z + yy
            s = hid_q[p, 0].astype(F32)
            for j in range(1, 4):
                s = s + in_qz[(z + j) % 4, yy].astype(F32)
            hid_q[p, 0] = s.astype(BF16)
        remote(hid_q.at[2 * z + 1 - y, 0], in_qy, cy_ss.at[0], cy_rs.at[0], over_y).start()

    def queries_end():
        got(in_qy, cy_rs.at[0])
        dhq[...] = (hid_q[2 * z + y, 0].astype(F32) + in_qy[...].astype(F32)).astype(BF16)

    def chip_sum(j):
        zs, p = pair_of(j)
        slot = j % 2
        got(hid_d.at[n_pair + p], bs_rs.at[p])

        @pl.loop(0, rd // 32)
        def _(t):
            r = pl.ds(pl.multiple_of(t * 32, 32), 32)
            hid_d[p, r] = (part[slot, c, r].astype(F32) + hid_d[n_pair + p, r].astype(F32)).astype(BF16)

        @pl.when(j % 2 == 0)
        def _():
            for h in range(2):
                r = pl.ds(h * half, half)
                remote(hid_d.at[p, r], in_y.at[zs, r], by_ss.at[zs, h], by_rs.at[zs, h], over_y).start()

    def line_step(e):
        k, h = 3 - e // 2, e % 2
        d = order(k)
        p = 2 * d + y
        r = pl.ds(h * half, half)
        from_left = jnp.logical_and(z > 0, d >= z)
        from_right = jnp.logical_and(z < 3, d <= z)
        left_slot = jnp.maximum(d - 1, 0)
        right_slot = jnp.minimum(d, 2)
        got(in_y.at[d, r], by_rs.at[d, h])
        acc[...] = hid_d[p, r].astype(F32) + in_y[d, r].astype(F32)

        @pl.when(from_left)
        def _():
            got(in_l.at[left_slot, r], bl_rs.at[d, h])
            acc[...] += in_l[left_slot, r].astype(F32)

        @pl.when(from_right)
        def _():
            got(in_r.at[right_slot, r], br_rs.at[d, h])
            acc[...] += in_r[right_slot, r].astype(F32)

        if k == 0:
            dhd[r] = acc[...].astype(BF16)
        else:
            hid_d[p, r] = acc[...].astype(BF16)

            @pl.when(d < z)
            def _():
                remote(hid_d.at[p, r], in_r.at[jnp.minimum(d, 2), r], bl_ss.at[d, h], br_rs.at[d, h], left).start()

            @pl.when(d > z)
            def _():
                remote(hid_d.at[p, r], in_l.at[jnp.maximum(d - 1, 0), r], br_ss.at[d, h], bl_rs.at[d, h], right).start()

    def weight_grad(n):
        cols = tile(n)

        @pl.loop(0, n_d // 8)
        def _(t):
            for i in range(8):
                d = t * 8 + i
                r = pl.ds(pl.multiple_of(d * d_len, 16), d_len)
                low[r, :] = (grad_d[pl.ds(d, 1), cols] * gate_d[r, cols]).astype(BF16)
        for q in range(0, n_q, 2):
            low[all_d + q_len * q:all_d + q_len * (q + 2), :] = two_queries(q, cols).astype(BF16)
        depth = all_d + NDEV * rq
        step = min(512, hidden)

        @pl.loop(0, hidden // step)
        def _(m):
            r = pl.ds(pl.multiple_of(m * step, step), step)
            dw[r, cols] = jnp.dot(hid_t[r, :], low[0:depth, :], preferred_element_type=F32).astype(BF16)

    @pl.loop(0, 9 + tiles)
    def _(u):
        @pl.when(jnp.logical_and(u < 9, u != 4))
        def _():
            j = u - u // 5
            slot = j % 2
            zs, p = pair_of(j)
            docs_gate(p)

            @pl.when(j >= 1)
            def _():
                chip_sum(j - 1)

            @pl.when(j >= 2)
            def _():
                sent(part.at[0, 0], bs_ss.at[slot])
            docs_hidden(slot)
            remote(part.at[slot, 1 - c], hid_d.at[n_pair + p], bs_ss.at[slot], bs_rs.at[p], sib).start()

        @pl.when(u == 4)
        def _():
            queries_back()

        @pl.when(u == 6)
        def _():
            queries_chip()

        @pl.when(u == 9)
        def _():
            chip_sum(7)
            queries_line()

        @pl.when(u >= 9)
        def _():
            weight_grad(u - 9)

        for e in range(8):
            at = END_AT[e] * (1 - mid) + MID_AT[e] * mid

            @pl.when(u == jnp.minimum(at, 8 + tiles))
            def _():
                line_step(e)

    queries_end()
    for slot in range(2):
        sent(part.at[0, 0], bs_ss.at[slot])
    sent(part_q.at[:, 0], cs_ss.at[0])
    for j in range(1, 4):
        sent(in_qz.at[0], cz_ss.at[j])
    sent(in_qy, cy_ss.at[0])
    for h in range(2):
        for zs in range(4):
            ref = in_y.at[0, pl.ds(0, half)]
            sent(ref, by_ss.at[zs, h])

            @pl.when(zs < z)
            def _():
                sent(ref, bl_ss.at[zs, h])

            @pl.when(zs > z)
            def _():
                sent(ref, br_ss.at[zs, h])


def solution(mesh):
    group_size = mesh.shape['tp']

    def device_step(query_hidden, doc_hidden, query_mask, doc_mask, positives, head_weight, head_bias):
        hidden, cols = head_weight.shape
        vocab_size = cols * group_size
        q_len = query_hidden.shape[1]
        d_len = doc_hidden.shape[1]
        lam_q = math.sqrt(d_len) / (4.0 * math.sqrt(vocab_size) * q_len)
        lam_d = q_len / (4.0 * math.sqrt(vocab_size) * d_len ** 1.5)
        rd, rq = ROWS * d_len, ROWS * q_len
        n_q = NDEV * ROWS
        all_d, all_q = NDEV * rd, NDEV * rq
        tiles = cols // TILE
        vmem = pl.BlockSpec(memory_space=pltpu.VMEM)
        hbm = pl.BlockSpec(memory_space=pl.ANY)
        dma = pltpu.SemaphoreType.DMA
        low_rows = max(tiles * max(all_q, 2 * rd), all_d + all_q)
        out = pl.pallas_call(
            functools.partial(kernel, d_len, q_len, lam_q, lam_d),
            out_shape=[
                jax.ShapeDtypeStruct((1, 1), F32),
                jax.ShapeDtypeStruct((hidden, cols), BF16),
                jax.ShapeDtypeStruct((1, cols), F32),
                jax.ShapeDtypeStruct((rd, hidden), BF16),
                jax.ShapeDtypeStruct((rq, hidden), BF16),
            ],
            in_specs=[hbm, hbm, vmem, vmem, pl.BlockSpec(memory_space=pltpu.SMEM), hbm, vmem],
            out_specs=[vmem] * 5,
            scratch_shapes=[
                pltpu.VMEM((NDEV, rd, hidden), BF16),
                pltpu.VMEM((NDEV // 2, 2, rq, hidden), BF16),
                pltpu.VMEM((NDEV, 16, TILE), BF16),
                pltpu.VMEM((hidden, cols), BF16),
                pltpu.VMEM((hidden, all_d + all_q), BF16),
                pltpu.VMEM((all_d, cols), F32),
                pltpu.VMEM((all_q, cols), F32),
                pltpu.VMEM((n_q, cols), F32),
                pltpu.VMEM((n_q, cols), F32),
                pltpu.VMEM((n_q, cols), F32),
                pltpu.VMEM((n_q, cols), F32),
                pltpu.VMEM((low_rows, TILE), BF16),
                pltpu.VMEM((2, 2, rd, hidden), BF16),
                pltpu.VMEM((NDEV // 2, 2, rq, hidden), BF16),
                pltpu.VMEM((4, rd, hidden), BF16),
                pltpu.VMEM((3, rd, hidden), BF16),
                pltpu.VMEM((3, rd, hidden), BF16),
                pltpu.VMEM((4, 2, rq, hidden), BF16),
                pltpu.VMEM((rq, hidden), BF16),
                pltpu.VMEM((rd // 2, hidden), F32),
                pltpu.VMEM((n_q, 128), F32),
                pltpu.VMEM((4, n_q, 128), F32),
                pltpu.VMEM((4, n_q, 128), F32),
                dma((3,)), dma((NDEV,)), dma((NDEV,)), dma((1,)), dma((1,)), dma((2, 4)), dma((4, 2)), dma((1,)), dma((1,)),
                dma((4, 2)), dma((4, 2)), dma((4, 2)), dma((4, 2)), dma((4, 2)), dma((8, 2)), dma((8, 2)),
                dma((4,)), dma((4,)), dma((4,)), dma((4,)),
                dma((2,)), dma((8,)), dma((4, 2)), dma((4, 2)), dma((4, 2)), dma((4, 2)), dma((4, 2)), dma((4, 2)),
                dma((1,)), dma((1,)), dma((4,)), dma((4,)), dma((1,)), dma((1,)),
            ],
            compiler_params=pltpu.CompilerParams(
                collective_id=0, has_side_effects=True, vmem_limit_bytes=67043328),
        )(doc_hidden.reshape(rd, hidden), query_hidden.reshape(rq, hidden), doc_mask, query_mask, positives,
          head_weight, head_bias)
        total_loss, grad_weight, grad_bias, grad_doc, grad_query = out
        return (total_loss.reshape(1), grad_weight, grad_bias,
                grad_query.reshape(query_hidden.shape), grad_doc.reshape(doc_hidden.shape))

    batch_rows = P(('dp', 'tp'), None, None)
    batch_masks = P(('dp', 'tp'), None)
    return jax.shard_map(device_step, mesh=mesh, in_specs=(batch_rows, batch_rows, batch_masks, batch_masks, P(('dp', 'tp')), P(None, 'tp'), P(None, 'tp')), out_specs=(P('dp'), P('dp', 'tp'), P('dp', 'tp'), batch_rows, batch_rows), check_vma=False)
```

```python
import functools
import math
import jax
import jax.numpy as jnp
from jax import lax
from jax.experimental import pallas as pl
from jax.experimental.pallas import tpu as pltpu
from jax.sharding import PartitionSpec as P

HIGHEST = lax.Precision.HIGHEST
F32 = jnp.float32
BF16 = jnp.bfloat16
TILE = 256
ROWS = 4
NDEV = 16
N_Z, SIDES = 4, 2
PAIR = SIDES * ROWS
OTHERS = (1, 2, 3)
DOWN = dict(axis=0, keepdims=True)
ACROSS = dict(axis=1, keepdims=True)
NT_DIMS = (((1,), (1,)), ((), ()))
TN_DIMS = (((0,), (0,)), ((), ()))

END_AT = (4, 5, 6, 8, 9, 11, 14, 16)
MID_AT = (8, 9, 11, 13, 11, 13, 15, 16)


def kernel(d_len, q_len, lam_q, lam_d,
           xd, xq, md, mq, pos, w, b,
           loss, dw_out, db, dhd, dhq,
           hid_d, hid_q, meta, meta_chip, wv, dw, hid_t, gate_d, gate_q, rep_d, rep_q,
           low, part, part_q, in_y, in_l, in_r, in_qz, in_qy, z_even, z_odd, pos_s, s_a, s_b,
           load_sem, out_sem, meta_ss, meta_rs, qy_ss, qy_rs, qz_ss, qz_rs, qs_ss, qs_rs,
           dl_ss, dr_ss, dz_rs, dy_ss, dy_rs, ds_ss, ds_rs,
           sa_ss, sa_rs, sb_ss, sb_rs,
           bs_ss, bs_rs, by_ss, by_rs, bl_ss, br_ss, bl_rs, br_rs,
           cs_ss, cs_rs, cz_ss, cz_rs, cy_ss, cy_rs):
    n_pair = NDEV // 2
    rd, rq = ROWS * d_len, ROWS * q_len
    half = rd // 2
    hidden = wv.shape[0]
    tiles = wv.shape[1] // TILE
    n_q, n_d = NDEV * ROWS, NDEV * ROWS
    all_d = NDEV * rd
    me = lax.axis_index('tp')
    z, y, c = me // 4, (me // 2) % 2, me % 2
    far = z // 2
    mid = z * (1 - far) + (3 - z) * far
    sib = me + 1 - 2 * c
    over_y = me + 2 - 4 * y
    left, right = me - 4, me + 4

    pair_rows = SIDES * rd
    rounds = N_Z * ROWS

    def spot(zs, yy):
        return SIDES * zs + yy

    def order(k):
        o = (k // 2) * k + (1 - k // 2) * ((k + mid) % 2)
        return o * (1 - far) + (3 - o) * far

    def remote(src, dst, ss, rs, dev):
        return pltpu.make_async_remote_copy(
            src_ref=src, dst_ref=dst, send_sem=ss, recv_sem=rs,
            device_id={'tp': dev}, device_id_type=pl.DeviceIdType.MESH)

    def got(dst, rs):
        remote(dst, dst, rs, rs, sib).wait_recv()

    def sent(src, ss):
        remote(src, src, ss, ss, sib).wait_send()

    def tile(n):
        return pl.ds(pl.multiple_of(n * TILE, TILE), TILE)

    fold = hidden // TILE

    def w_block(n, first, size):
        return pl.ds((n % fold) * TILE, TILE), pl.ds(pl.multiple_of((n // fold) * hidden + first, TILE), size)

    def transpose_weight():
        @pl.loop(0, hidden // TILE)
        def _(t):
            for n in range(tiles):
                r, l = w_block(n, t * TILE, TILE)
                dw[r, l] = wv[tile(t), n * TILE:(n + 1) * TILE].T

    load_d = pltpu.make_async_copy(xd, hid_d.at[me], load_sem.at[0])
    load_q = pltpu.make_async_copy(xq, hid_q.at[me // 2, c], load_sem.at[1])
    load_w = pltpu.make_async_copy(w, wv, load_sem.at[2])
    load_d.start()
    load_q.start()
    load_w.start()
    barrier = pltpu.get_barrier_semaphore()
    line = [(me + 4 * j) % NDEV for j in OTHERS]
    quad = 2 * y + c
    plane = [4 * z + (quad + j) % 4 for j in OTHERS]
    for dev in line + plane:
        pl.semaphore_signal(barrier, inc=1, device_id={'tp': dev}, device_id_type=pl.DeviceIdType.MESH)
    row16 = lax.broadcasted_iota(jnp.int32, (16, TILE), 0)
    own_meta = jnp.zeros((16, TILE), F32)
    for r in range(ROWS):
        len_d = jnp.sum(md[r:r + 1, :].astype(F32), **ACROSS)
        len_q = jnp.sum(mq[r:r + 1, :].astype(F32), **ACROSS)
        own_meta = jnp.where(row16 == r, len_d, own_meta)
        own_meta = jnp.where(row16 == ROWS + r, len_q, own_meta)
        own_meta = jnp.where(row16 == PAIR + r, pos[r].astype(F32), own_meta)
    own_meta = own_meta.astype(BF16)
    meta[z, y, c] = own_meta
    meta_chip[c] = own_meta
    load_w.wait()
    transpose_weight()
    load_d.wait()
    load_q.wait()
    pl.semaphore_wait(barrier, 6)

    def doc(shard, q):
        return hid_d.at[shard, pl.ds(pl.multiple_of(q * d_len, 16), d_len)]

    def to_sib(p, q):
        ref = doc(SIDES * p + c, q)
        remote(ref, ref, ds_ss.at[p, q], ds_rs.at[p, q], sib).start()

    def pass_on(zs, q):
        ref = doc(SIDES * spot(zs, y) + c, q)

        @pl.when(jnp.logical_and(zs >= z, z > 0))
        def _():
            remote(ref, ref, dl_ss.at[zs, q], dz_rs.at[zs, q], left).start()

        @pl.when(jnp.logical_and(zs <= z, z < 3))
        def _():
            remote(ref, ref, dr_ss.at[zs, q], dz_rs.at[zs, q], right).start()

        remote(ref, ref, dy_ss.at[zs, q], dy_rs.at[zs, q], over_y).start()
        to_sib(spot(zs, y), q)

    def arrive_line(k, q):
        zs = order(k)
        got(doc(SIDES * spot(zs, y) + c, q), dz_rs.at[zs, q])
        pass_on(zs, q)

    def arrive_over(k, q):
        zs = order(k)
        p = spot(zs, 1 - y)
        got(doc(SIDES * p + c, q), dy_rs.at[zs, q])
        to_sib(p, q)

    def query_out(yy):
        ref = hid_q.at[spot(z, yy), c]
        for j in OTHERS:
            remote(ref, ref, qz_ss.at[yy, j], qz_rs.at[z, yy], (me + 4 * j) % NDEV).start()

    def meta_over():
        for j in OTHERS:
            zs = (z + j) % N_Z
            got(meta.at[zs, y, c], meta_rs.at[zs])
        remote(meta.at[:, y, c], meta.at[:, y, c], meta_ss.at[4], meta_rs.at[4], over_y).start()

    def meta_share():
        got(meta.at[:, 1 - y, c], meta_rs.at[4])
        remote(meta.at[:, :, c], meta.at[:, :, c], meta_ss.at[5], meta_rs.at[5], sib).start()

    own_q = hid_q.at[me // 2, c]
    remote(meta_chip.at[c], meta_chip.at[c], meta_ss.at[0], meta_rs.at[6], sib).start()
    for j in OTHERS:
        remote(meta.at[z, y, c], meta.at[z, y, c], meta_ss.at[j], meta_rs.at[z], line[j - 1]).start()
    pass_on(z, 0)
    for q in range(1, ROWS):
        pass_on(z, q)
    remote(own_q, own_q, qy_ss.at[0], qy_rs.at[0], over_y).start()

    @pl.when(mid == 0)
    def _():
        query_out(y)

    def arrivals(e):
        g, q = e // ROWS, e % ROWS

        @pl.when(mid == 0)
        def _():
            @pl.when(g < 3)
            def _():
                arrive_line(g + 1, q)

        @pl.when(mid == 1)
        def _():
            @pl.when(g == 0)
            def _():
                arrive_line(1, q)
                arrive_line(2, q)

            @pl.when(g == 1)
            def _():
                arrive_line(3, q)

        arrive_over(g, q)

        @pl.when(e == PAIR - 1)
        def _():
            @pl.when(mid == 1)
            def _():
                query_out(y)
            got(hid_q.at[spot(z, 1 - y), c], qy_rs.at[0])
            query_out(1 - y)

    def pump(v):
        last = jnp.minimum(v + 3, rounds) - 2 * (1 // (v + 1))

        @pl.loop(jnp.minimum(v + 2 * jnp.minimum(v // 2, 1), rounds), last)
        def _(e):
            arrivals(e)

        pl.when(v == 0)(meta_over)
        pl.when(v == 1)(meta_share)

    got(meta_chip.at[1 - c], meta_rs.at[6])

    def gated(logits, cap):
        held = jnp.maximum(jnp.minimum(logits, cap), 0.0)
        up = 1.0 + held
        inv = 1.0 / up
        act = jnp.log(up) + (held - (up - 1.0)) * inv
        return act, jnp.where(held > 0.0, inv, 0.0)

    place_d = lax.broadcasted_iota(jnp.int32, (d_len, 128), 0).astype(F32)
    place_q = lax.broadcasted_iota(jnp.int32, (q_len, 128), 0).astype(F32)

    def cap_of(place, length):
        cap = jnp.where(place < length, jnp.finfo(F32).max, 0.0)
        return jnp.concatenate([cap, cap], axis=1)

    def forward(rows, load, finish, transpose, beside):
        def product(n, z_ref):
            z_ref[0:rows, :] = jnp.dot(load(), wv[:, tile(n)], preferred_element_type=F32)

        product(0, z_even)

        @pl.loop(0, tiles // 2)
        def _(i):
            n = 2 * i
            product(n + 1, z_odd)
            finish(n, z_even)
            transpose(n)
            product(jnp.minimum(n + 2, tiles - 1), z_even)
            finish(n + 1, z_odd)
            transpose(n + 1)
            beside(i)

    lane_step = hidden // tiles

    def docs_forward(p, beside):
        info = meta_chip[...].astype(F32)

        def load():
            return hid_d[pl.ds(SIDES * p, SIDES)].reshape(pair_rows, hidden)

        def finish(n, z_ref):
            cols = tile(n)
            bias = b[:, cols]
            for d in range(PAIR):
                cap = cap_of(place_d, info[d // ROWS, d % ROWS:d % ROWS + 1, 0:128])
                act, gate = gated(z_ref[d_len * d:d_len * (d + 1), :] + bias, cap)
                gate_d[pl.ds(p * pair_rows + d_len * d, d_len), cols] = gate
                rep_d[pl.ds(p * PAIR + d, 1), cols] = jnp.sum(act, **DOWN)

        def transpose(n):
            lanes = pl.ds(pl.multiple_of(n * lane_step, lane_step), lane_step)
            block = hid_d[pl.ds(SIDES * p, SIDES), :, lanes].reshape(pair_rows, lane_step)
            hid_t[lanes, pl.ds(pl.multiple_of(p * pair_rows, 128), pair_rows)] = block.T

        forward(pair_rows, load, finish, transpose, beside)

    def queries_forward():
        def load():
            return hid_q[...].reshape(NDEV * rq, hidden)

        def finish(n, z_ref):
            cols = tile(n)
            bias = b[:, cols]
            for i in range(NDEV):
                info = meta[i // N_Z, (i // SIDES) % SIDES, i % SIDES].astype(F32)
                for r in range(ROWS):
                    q = ROWS * i + r
                    cap = cap_of(place_q, info[ROWS + r:ROWS + r + 1, 0:128])
                    act, gate = gated(z_ref[q_len * q:q_len * (q + 1), :] + bias, cap)
                    gate_q[q_len * q:q_len * (q + 1), cols] = gate
                    rep_q[q:q + 1, cols] = jnp.sum(act, **DOWN)

        def transpose(n):
            lanes = pl.ds(pl.multiple_of(n * lane_step, lane_step), lane_step)
            block = hid_q[:, :, :, lanes].reshape(NDEV * rq, lane_step)
            hid_t[lanes, all_d:all_d + NDEV * rq] = block.T

        forward(NDEV * rq, load, finish, transpose, lambda i: None)

    def queries_share():
        for j in OTHERS:
            zs = (z + j) % N_Z
            for yy in range(SIDES):
                got(hid_q.at[spot(zs, yy), c], qz_rs.at[zs, yy])
        remote(hid_q.at[:, c], hid_q.at[:, c], qs_ss.at[0], qs_rs.at[0], sib).start()

    every = max(tiles // 4, 1)

    @pl.loop(0, n_pair)
    def _(u):
        end, odd, some = u // 7, u % 2, (u + 6) // 7
        other = end + (1 - end) * (1 - odd) * some
        k = end * 3 + (1 - end) * (odd * ((u + 1) // 2) + (1 - odd) * some * (u // 2 - 1))
        p = 2 * order(k) + y + other * (1 - 2 * y)

        @pl.when(u == 7)
        def _():
            queries_share()

        for q in range(ROWS):
            got(doc(SIDES * p + 1 - c, q), ds_rs.at[p, q])

        def beside(i):
            @pl.when(i % every == every - 1)
            def _():
                pump(2 * u + i // every)

        @pl.when(u == 1)
        def _():
            got(meta.at[:, :, 1 - c], meta_rs.at[5])

        @pl.when(u > 0)
        def _():
            meta_chip[...] = meta[p // 2, p % 2]
        docs_forward(p, beside)

        @pl.when(u == 0)
        def _():
            sent(meta_chip.at[c], meta_ss.at[0])

    got(hid_q.at[:, 1 - c], qs_rs.at[0])
    queries_forward()

    for j in OTHERS:
        sent(meta.at[z, y, c], meta_ss.at[j])
    sent(meta.at[:, y, c], meta_ss.at[4])
    sent(meta.at[:, :, c], meta_ss.at[5])
    sent(own_q, qy_ss.at[0])
    for yy in range(SIDES):
        for j in OTHERS:
            sent(own_q, qz_ss.at[yy, j])
    sent(hid_q.at[:, c], qs_ss.at[0])
    for q in range(ROWS):
        ref = doc(me, q)
        for zs in range(4):
            sent(ref, dy_ss.at[zs, q])

            @pl.when(jnp.logical_and(zs >= z, z > 0))
            def _():
                sent(ref, dl_ss.at[zs, q])

            @pl.when(jnp.logical_and(zs <= z, z < 3))
            def _():
                sent(ref, dr_ss.at[zs, q])
        for p in range(n_pair):
            sent(ref, ds_ss.at[p, q])

    mean_q = jnp.mean(rep_q[...], **DOWN)
    mean_d = jnp.mean(rep_d[...], **DOWN)
    reg = (lam_q * jnp.sum(mean_q * mean_q, **ACROSS)
           + lam_d * jnp.sum(mean_d * mean_d, **ACROSS))
    hq = n_q // 2
    part_s = lax.dot_general(rep_q[...], rep_d[...], NT_DIMS, precision=HIGHEST, preferred_element_type=F32)
    s_a[quad, 0:hq, 0:n_d] = part_s[0:hq]
    s_a[quad, 0:hq, n_d:128] = part_s[hq:n_q]
    s_a[quad, hq:hq + 8, :] = jnp.broadcast_to(reg, (8, 128))
    for j in OTHERS:
        remote(s_a.at[quad], s_a.at[quad], sa_ss.at[j], sa_rs.at[quad], plane[j - 1]).start()
    for i in range(NDEV):
        info = meta[i // N_Z, (i // SIDES) % SIDES, i % SIDES].astype(F32)
        pos_s[ROWS * i:ROWS * (i + 1), :] = info[PAIR:3 * ROWS, 0:128]
    for j in OTHERS:
        src = (quad + j) % 4
        got(s_a.at[src], sa_rs.at[src])
    s_b[z] = s_a[0] + s_a[1] + s_a[2] + s_a[3]
    for j in OTHERS:
        remote(s_b.at[z], s_b.at[z], sb_ss.at[j], sb_rs.at[z], line[j - 1]).start()
    for j in OTHERS:
        src = (z + j) % N_Z
        got(s_b.at[src], sb_rs.at[src])
    total = s_b[0] + s_b[1] + s_b[2] + s_b[3]
    scores = jnp.concatenate([total[0:hq, 0:n_d], total[0:hq, n_d:128]], axis=0)
    top = jnp.max(scores, **ACROSS)
    log_norm = top + jnp.log(jnp.sum(jnp.exp(scores - top), **ACROSS))
    lane = lax.broadcasted_iota(jnp.int32, (n_q, n_d), 1).astype(F32)
    target = (pos_s[:, 0:n_d] == lane).astype(F32)
    picked = jnp.sum(target * scores, **ACROSS)
    cross = jnp.sum(log_norm - picked, **DOWN) / n_q
    loss[...] = cross + total[hq:hq + 1, 0:1]
    grad_s = (jnp.exp(scores - log_norm) - target) / n_q

    @pl.loop(0, tiles)
    def _(n):
        cols = tile(n)
        rep_qn, rep_dn = rep_q[:, cols], rep_d[:, cols]
        back_q = lax.dot_general(
            grad_s, rep_dn, (((1,), (0,)), ((), ())), precision=HIGHEST, preferred_element_type=F32
        ) + (2.0 * lam_q / n_q) * jnp.mean(rep_qn, **DOWN)
        back_d = lax.dot_general(
            grad_s, rep_qn, TN_DIMS, precision=HIGHEST, preferred_element_type=F32
        ) + (2.0 * lam_d / n_d) * jnp.mean(rep_dn, **DOWN)
        rep_q[:, cols] = back_q
        rep_d[:, cols] = back_d

    db[...] = jnp.zeros_like(db)
    for j in OTHERS:
        sent(s_a.at[0], sa_ss.at[j])
        sent(s_b.at[0], sb_ss.at[j])

    grad_q, grad_d = rep_q, rep_d
    bufs = (low, wv)

    def pair_of(j):
        end, odd, some = j // 7, j % 2, (j + 6) // 7
        other = odd * (1 - end) + (1 - odd) * (1 - some)
        k = odd * ((7 - j) // 2 - 1 + end) + (1 - odd) * (4 - j // 2 - (1 - some))
        zs = order(k)
        return other, zs, spot(zs, y) + other * (1 - 2 * y)

    def hidden_grad(rows, buf, store, beside):
        @pl.loop(0, hidden // TILE)
        def _(t):
            out = jnp.zeros((rows, TILE), F32)
            for n in range(tiles):
                r, l = w_block(n, t * TILE, TILE)
                out = out + jnp.dot(buf[0:rows, n * TILE:(n + 1) * TILE], dw[r, l],
                                    preferred_element_type=F32)
            store(tile(t), out.astype(BF16))
            beside(t)

    def docs_gate(p, buf, n):
        cols = tile(n)
        total_b = jnp.zeros((1, TILE), F32)
        for d in range(PAIR):
            gz = (grad_d[pl.ds(PAIR * p + d, 1), cols]
                  * gate_d[pl.ds(p * pair_rows + d_len * d, d_len), cols])
            total_b = total_b + jnp.sum(gz, **DOWN)
            buf[d_len * d:d_len * (d + 1), cols] = gz.astype(BF16)
        db[:, cols] += total_b

    def docs_hidden(slot, beside):
        def store(hrows, out):
            part[slot, :, :, hrows] = out.reshape(2, rd, TILE)
        hidden_grad(pair_rows, bufs[slot], store, beside)

    def two_queries(q, cols):
        return jnp.concatenate(
            [grad_q[q + i:q + i + 1, cols] * gate_q[q_len * (q + i):q_len * (q + i + 1), cols]
             for i in range(SIDES)], axis=0)

    def queries_back():
        buf = bufs[0]

        @pl.loop(0, tiles)
        def _(n):
            cols = tile(n)
            total_b = jnp.zeros((1, TILE), F32)
            for q in range(0, n_q, 2):
                gz = two_queries(q, cols)
                total_b = total_b + jnp.sum(gz, **DOWN)
                buf[q_len * q:q_len * (q + 2), cols] = gz.astype(BF16)
            db[:, cols] += total_b

        chip_sum(0)

        def store(hrows, out):
            part_q[:, :, :, hrows] = out.reshape(n_pair, 2, rq, TILE)
        hidden_grad(NDEV * rq, buf, store, lambda t: None)
        remote(part_q.at[:, 1 - c], hid_q.at[:, 1], cs_ss.at[0], cs_rs.at[0], sib).start()

    def queries_chip():
        got(hid_q.at[:, 1], cs_rs.at[0])

        @pl.loop(0, n_pair)
        def _(p):
            hid_q[p, 0] = (part_q[p, c].astype(F32) + hid_q[p, 1].astype(F32)).astype(BF16)
        for j in OTHERS:
            zs = (z + j) % N_Z
            remote(hid_q.at[pl.ds(2 * zs, 2), 0], in_qz.at[z], cz_ss.at[j], cz_rs.at[z],
                   (me + 4 * j) % NDEV).start()

    def queries_line():
        for j in OTHERS:
            src = (z + j) % N_Z
            got(in_qz.at[src], cz_rs.at[src])
        for yy in range(SIDES):
            p = spot(z, yy)
            s = hid_q[p, 0].astype(F32)
            for j in OTHERS:
                s = s + in_qz[(z + j) % N_Z, yy].astype(F32)
            hid_q[p, 0] = s.astype(BF16)
        remote(hid_q.at[spot(z, 1 - y), 0], in_qy, cy_ss.at[0], cy_rs.at[0], over_y).start()

    def queries_end():
        got(in_qy, cy_rs.at[0])
        dhq[...] = (hid_q[spot(z, y), 0].astype(F32) + in_qy[...].astype(F32)).astype(BF16)

    def chip_sum(j):
        other, zs, p = pair_of(j)
        slot = j % 2
        got(hid_d.at[n_pair + p], bs_rs.at[p])

        @pl.loop(0, rd // 32)
        def _(t):
            r = pl.ds(pl.multiple_of(t * 32, 32), 32)
            hid_d[p, r] = (part[slot, c, r].astype(F32) + hid_d[n_pair + p, r].astype(F32)).astype(BF16)

        @pl.when(other == 1)
        def _():
            for h in range(SIDES):
                r = pl.ds(h * half, half)
                remote(hid_d.at[p, r], in_y.at[zs, r], by_ss.at[zs, h], by_rs.at[zs, h], over_y).start()

    def line_step(e):
        k, h = 3 - e // 2, e % 2
        d = order(k)
        p = spot(d, y)
        r = pl.ds(h * half, half)
        from_left = jnp.logical_and(z > 0, d >= z)
        from_right = jnp.logical_and(z < 3, d <= z)
        left_slot = jnp.maximum(d - 1, 0)
        right_slot = jnp.minimum(d, 2)
        got(in_y.at[d, r], by_rs.at[d, h])

        @pl.when(from_left)
        def _():
            got(in_l.at[left_slot, r], bl_rs.at[d, h])

        @pl.when(from_right)
        def _():
            got(in_r.at[right_slot, r], br_rs.at[d, h])

        def add(*terms):
            @pl.loop(0, half // 16)
            def _(i):
                q = pl.ds(pl.multiple_of(h * half + i * 16, 16), 16)
                s = hid_d[p, q].astype(F32) + in_y[d, q].astype(F32)
                for ref, slot in terms:
                    s = s + ref[slot, q].astype(F32)
                if k == 0:
                    dhd[q] = s.astype(BF16)
                else:
                    hid_d[p, q] = s.astype(BF16)

        both = jnp.logical_and(from_left, from_right)
        pl.when(both)(lambda: add((in_l, left_slot), (in_r, right_slot)))
        pl.when(jnp.logical_and(from_left, jnp.logical_not(from_right)))(lambda: add((in_l, left_slot)))
        pl.when(jnp.logical_and(from_right, jnp.logical_not(from_left)))(lambda: add((in_r, right_slot)))
        pl.when(jnp.logical_not(jnp.logical_or(from_left, from_right)))(lambda: add())
        if k > 0:
            @pl.when(d < z)
            def _():
                remote(hid_d.at[p, r], in_r.at[jnp.minimum(d, 2), r], bl_ss.at[d, h], br_rs.at[d, h], left).start()

            @pl.when(d > z)
            def _():
                remote(hid_d.at[p, r], in_l.at[jnp.maximum(d - 1, 0), r], br_ss.at[d, h], bl_rs.at[d, h], right).start()

    depth = NDEV * rq
    blocks = (all_d + depth) // depth
    steps = max(hidden // 512, 1)

    def weight_gate(n, buf, m):
        cols = tile(n)
        share = n_d // steps

        for i in range(share):
            d = m * share + i
            r = pl.ds(pl.multiple_of(d * d_len, 16), d_len)
            gz = (grad_d[pl.ds(d, 1), cols] * gate_d[r, cols]).astype(BF16)
            for piece in range(0, d_len, 16):
                at = m * share * d_len + i * d_len + piece
                blk, row = at // depth, at % depth
                buf[pl.ds(pl.multiple_of(row, 16), 16), tile(blk)] = gz[piece:piece + 16]

    def weight_gate_q(n, buf):
        cols = tile(n)
        for q in range(0, n_q, 2):
            buf[q_len * q:q_len * (q + 2), (blocks - 1) * TILE:blocks * TILE] = two_queries(q, cols).astype(BF16)

    def weight_grad(n, slot, ahead):
        cols = tile(n)
        size = hidden // steps
        for m in range(steps):
            r = slice(m * size, (m + 1) * size)
            out = jnp.zeros((size, TILE), F32)
            for i in range(blocks):
                out = out + jnp.dot(hid_t[r, i * depth:(i + 1) * depth],
                                    bufs[slot][0:depth, i * TILE:(i + 1) * TILE], preferred_element_type=F32)
            dw[r, cols] = out.astype(BF16)
            pltpu.make_async_copy(dw.at[r, cols], dw_out.at[r, cols], out_sem.at[m, n]).start()
            weight_gate(ahead, bufs[1 - slot], m)
        weight_gate_q(ahead, bufs[1 - slot])

    pair_tiles = tiles // (hidden // TILE)

    def gate_next(j, slot, t):
        _, _, p = pair_of(j)
        for i in range(pair_tiles):
            docs_gate(p, bufs[slot], t * pair_tiles + i)

    @pl.loop(0, hidden // TILE)
    def _(t):
        gate_next(0, 0, t)

    @pl.loop(0, 9 + tiles)
    def _(u):
        is_pair = jnp.logical_and(u < 9, u != 1)
        j = u - jnp.minimum(u, 1)
        for slot in range(SIDES):
            @pl.when(jnp.logical_and(is_pair, j % 2 == slot))
            def _():
                _, _, p = pair_of(j)

                @pl.when(j >= 2)
                def _():
                    sent(part.at[0, 0], bs_ss.at[slot])
                if slot == 0:
                    docs_hidden(0, lambda t: gate_next(j + 1, 1, t))
                else:
                    @pl.when(j < 7)
                    def _():
                        docs_hidden(1, lambda t: gate_next(j + 1, 0, t))

                    @pl.when(j == 7)
                    def _():
                        docs_hidden(1, lambda t: None)
                remote(part.at[slot, 1 - c], hid_d.at[n_pair + p], bs_ss.at[slot], bs_rs.at[p], sib).start()

                @pl.when(j >= 2)
                def _():
                    chip_sum(j - 1)

        @pl.when(u == 1)
        def _():
            queries_back()

        @pl.when(u == 2)
        def _():
            queries_chip()

        @pl.when(u == 9)
        def _():
            for m in range(steps):
                weight_gate(0, bufs[1], m)
            weight_gate_q(0, bufs[1])
            chip_sum(7)

        for slot in range(SIDES):
            @pl.when(jnp.logical_and(u >= 9, u % 2 == slot))
            def _():
                n = u - 9
                weight_grad(n, slot, jnp.minimum(n + 1, tiles - 1))

        @pl.when(u == 13)
        def _():
            queries_line()

        for e in range(8):
            at = END_AT[e] * (1 - mid) + MID_AT[e] * mid

            @pl.when(u == jnp.minimum(at, 8 + tiles))
            def _():
                line_step(e)

    queries_end()
    for m in range(steps):
        for n in range(tiles):
            r = slice(m * (hidden // steps), (m + 1) * (hidden // steps))
            l = slice(n * TILE, (n + 1) * TILE)
            pltpu.make_async_copy(dw.at[r, l], dw_out.at[r, l], out_sem.at[m, n]).wait()
    for slot in range(SIDES):
        sent(part.at[0, 0], bs_ss.at[slot])
    sent(part_q.at[:, 0], cs_ss.at[0])
    for j in OTHERS:
        sent(in_qz.at[0], cz_ss.at[j])
    sent(in_qy, cy_ss.at[0])
    for h in range(SIDES):
        for zs in range(4):
            ref = in_y.at[0, pl.ds(0, half)]
            sent(ref, by_ss.at[zs, h])

            @pl.when(zs < z)
            def _():
                sent(ref, bl_ss.at[zs, h])

            @pl.when(zs > z)
            def _():
                sent(ref, br_ss.at[zs, h])


def hand_over(dw, db, dhd, dhq, dw_out, db_out, dhd_out, dhq_out, buf_w, buf_b, buf_d, buf_q, read, write):
    steps = 8
    rows = dw.shape[0] // steps
    moves = [(dw.at[pl.ds(i * rows, rows)], buf_w.at[pl.ds(i * rows, rows)], dw_out.at[pl.ds(i * rows, rows)])
             for i in range(steps)]
    moves += [(dhd, buf_d, dhd_out), (dhq, buf_q, dhq_out), (db, buf_b, db_out)]
    for i, (src, buf, dst) in enumerate(moves):
        pltpu.make_async_copy(src, buf, read.at[i]).start()
    for i, (src, buf, dst) in enumerate(moves):
        pltpu.make_async_copy(src, buf, read.at[i]).wait()
        pltpu.make_async_copy(buf, dst, write.at[i]).start()
    for i, (src, buf, dst) in enumerate(moves):
        pltpu.make_async_copy(buf, dst, write.at[i]).wait()


def solution(mesh):
    group_size = mesh.shape['tp']

    def device_step(query_hidden, doc_hidden, query_mask, doc_mask, positives, head_weight, head_bias):
        hidden, cols = head_weight.shape
        vocab_size = cols * group_size
        q_len = query_hidden.shape[1]
        d_len = doc_hidden.shape[1]
        lam_q = math.sqrt(d_len) / (4.0 * math.sqrt(vocab_size) * q_len)
        lam_d = q_len / (4.0 * math.sqrt(vocab_size) * d_len ** 1.5)
        rd, rq = ROWS * d_len, ROWS * q_len
        n_q = NDEV * ROWS
        all_d, all_q = NDEV * rd, NDEV * rq
        pair_rows = SIDES * rd
        vmem = pl.BlockSpec(memory_space=pltpu.VMEM)
        hbm = pl.BlockSpec(memory_space=pl.ANY)
        dma = pltpu.SemaphoreType.DMA
        one, few = dma((1,)), dma((NDEV // SIDES,))
        out_y, in_z = dma((SIDES, N_Z)), dma((N_Z, SIDES))
        by_doc, all_docs, by_half = dma((N_Z, ROWS)), dma((NDEV // SIDES, ROWS)), dma((N_Z, SIDES))
        out = pl.pallas_call(
            functools.partial(kernel, d_len, q_len, lam_q, lam_d),
            out_shape=[
                jax.ShapeDtypeStruct((1, 1), F32),
                jax.ShapeDtypeStruct((hidden, cols), BF16),
                jax.ShapeDtypeStruct((1, cols), F32),
                jax.ShapeDtypeStruct((rd, hidden), BF16),
                jax.ShapeDtypeStruct((rq, hidden), BF16),
            ],
            in_specs=[hbm, hbm, vmem, vmem, pl.BlockSpec(memory_space=pltpu.SMEM), hbm, vmem],
            out_specs=[vmem, hbm, vmem, vmem, vmem],
            scratch_shapes=[
                pltpu.VMEM((NDEV, rd, hidden), BF16),
                pltpu.VMEM((NDEV // 2, 2, rq, hidden), BF16),
                pltpu.VMEM((N_Z, SIDES, SIDES, 16, TILE), BF16),
                pltpu.VMEM((2, 16, TILE), BF16),
                pltpu.VMEM((hidden, cols), BF16),
                pltpu.VMEM((hidden, cols), BF16),
                pltpu.VMEM((hidden, all_d + all_q), BF16),
                pltpu.VMEM((all_d, cols), F32),
                pltpu.VMEM((all_q, cols), F32),
                pltpu.VMEM((n_q, cols), F32),
                pltpu.VMEM((n_q, cols), F32),
                pltpu.VMEM((max(all_q, pair_rows), cols), BF16),
                pltpu.VMEM((2, 2, rd, hidden), BF16),
                pltpu.VMEM((NDEV // 2, 2, rq, hidden), BF16),
                pltpu.VMEM((4, rd, hidden), BF16),
                pltpu.VMEM((3, rd, hidden), BF16),
                pltpu.VMEM((3, rd, hidden), BF16),
                pltpu.VMEM((4, 2, rq, hidden), BF16),
                pltpu.VMEM((rq, hidden), BF16),
                pltpu.VMEM((max(all_q, pair_rows), TILE), F32),
                pltpu.VMEM((max(all_q, pair_rows), TILE), F32),
                pltpu.VMEM((n_q, 128), F32),
                pltpu.VMEM((4, n_q // 2 + 8, 128), F32),
                pltpu.VMEM((4, n_q // 2 + 8, 128), F32),
                few, dma((max(hidden // 512, 1), cols // TILE)), few, few, one, one, out_y, in_z, one, one,
                by_doc, by_doc, by_doc, by_doc, by_doc, all_docs, all_docs,
                few, few, few, few,
                few, few, by_half, by_half, by_half, by_half, by_half, by_half,
                one, one, few, few, one, one,
            ],
            compiler_params=pltpu.CompilerParams(
                collective_id=0, has_side_effects=True, vmem_limit_bytes=67043328),
        )(doc_hidden.reshape(rd, hidden), query_hidden.reshape(rq, hidden), doc_mask, query_mask, positives,
          head_weight, head_bias)
        total_loss = out[0]
        grad_weight, grad_bias, grad_doc, grad_query = pl.pallas_call(
            hand_over,
            out_shape=[jax.ShapeDtypeStruct(x.shape, x.dtype) for x in out[1:]],
            in_specs=[hbm] * 4,
            out_specs=[hbm] * 4,
            scratch_shapes=[pltpu.VMEM(x.shape, x.dtype) for x in out[1:]] + [dma((11,)), dma((11,))],
        )(*out[1:])
        return (total_loss.reshape(1), grad_weight, grad_bias,
                grad_query.reshape(query_hidden.shape), grad_doc.reshape(doc_hidden.shape))

    batch_rows = P(('dp', 'tp'), None, None)
    batch_masks = P(('dp', 'tp'), None)
    return jax.shard_map(device_step, mesh=mesh, in_specs=(batch_rows, batch_rows, batch_masks, batch_masks, P(('dp', 'tp')), P(None, 'tp'), P(None, 'tp')), out_specs=(P('dp'), P('dp', 'tp'), P('dp', 'tp'), batch_rows, batch_rows), check_vma=False)
```
